32 devices in a mesh: tm: 8 (over z, y), col: 4 (over x, core).
Axes of the slice: x: 2, y: 2, z: 4, core: 2. Of those that a mesh axis runs over, the one named last changes fastest.
Arguments:
- block_values: bfloat16 [4, 16384, 128], P('col', 'tm'), may hold values from -6 to 6
- block_shifts: bfloat16 [4, 16384, 128], P('col', 'tm'), may hold values from -1 to 1
- block_sensor: int32 [4, 16384], P('col', 'tm'), may hold values from 0 to 4095
- block_window: int32 [4, 16384], P('col', 'tm'), may hold values from 0 to 3
- block_owner: int32 [4, 16384, 1], P('col', 'tm'), may hold values from 0 to 7; in each aligned block of 2048 rows (0 to 2047, 2048 to 4095, ..., all dimensions but the last counted through in order) at most 384 rows name the same one
- block_counts: int32 [4, 8], P('col', 'tm'), may hold values from 1536 to 2048
- calibration: bfloat16 [16384, 4096], P('tm', 'col'), may hold values from -0.046875 to 0.046875
Outputs:
- calibrated: bfloat16 [4096, 4096], P('tm', 'col')
The draws below stay inside these ranges and needn't reach their ends.
Inputs may be any that keep to these rules, and one draw needn't show every extreme that they name: `block_owner`: among the 2048 block slots of one device, at most 384 name the same owner, a bound that some block reaches. The live blocks of device (tm t, col c) are its first block_counts[c, t] slots.
All inputs are finite; a program needn't handle non-finite values.
Results may differ from the reference program's by a relative error of at most 0.015.
Values may be sent and summed in bfloat16 or wider, within the bound.
No kernel may reach another device: no remote copies, remote signals or barrier semaphores. Data moves between devices by JAX's collectives and lax.ppermute only.
A program may use at most 128 MiB of HBM per device.

```python
import math
import jax
import jax.numpy as jnp
import numpy as np
from jax import lax

SENSORS = 16384
OUTPUTS = 4096
BLOCK_LEN = 128
BLOCKS_DEV = 2048
WINDOWS = 4
CAPACITY = 384
GROUP_SENSORS = 4096
BLOCK_ROWS = 16384
GRID_ROWS = 4096
N_TM = 8
N_COL = 4


def plant(drawn, key, low, high):
    extent = drawn.shape
    index_at = [jax.random.randint(jax.random.fold_in(key, axis), (), 0, extent[axis]) for axis in range(len(extent))]
    drawn = drawn.at[tuple(index_at)].set(low)
    longest = extent.index(max(extent))
    index_at[longest] = (index_at[longest] + 1) % extent[longest]
    return drawn.at[tuple(index_at)].set(high)


def steps_of(key, dims, shards, low, top_value):
    level, own = 1.0, jax.random.fold_in(key, 6)
    for dim, blocks in shards:
        draws = jnp.exp(jax.random.uniform(jax.random.fold_in(own, dim), (blocks,), jnp.float32, low / len(shards), top_value / len(shards)))
        level = level * jnp.repeat(draws, dims[dim] // blocks).reshape([-1 if axis == dim else 1 for axis in range(len(dims))])
    return level


def deal_out(stream_key, own, number, rows, count, top, reach, slope):
    sequence = jax.random.permutation(stream_key, count)
    packed, usual = load_shares(count, rows * top, reach, slope, True), load_shares(count, rows * top, reach, slope, False)
    places = jnp.arange(count)

    def named(lengths, offset_by):
        used = int((lengths > 0).sum())
        fixed = max(1, used // 4)
        shifted = fixed + (places - fixed + offset_by * (used - fixed)) % max(1, count - fixed)
        return jnp.zeros((count,), jnp.int32).at[sequence[jnp.where(places < fixed, places, shifted)]].set(jnp.asarray(lengths, jnp.int32))

    lengths = jnp.where(number % 4 == 0, named(packed, number // 4), named(usual, number - number // 4 - 1))
    mixed = jax.random.permutation(jax.random.fold_in(own, 3), count)
    donor, sink = mixed[0:count // 2 * 2:2], mixed[1:count // 2 * 2:2]
    margin = jnp.minimum(lengths[donor] - 1, reach - lengths[sink]) // 2
    margin = jnp.where((donor == sequence[0]) | (sink == sequence[0]) | (lengths[sink] == 0), 0, jnp.maximum(margin, 0))
    shifted = jax.random.randint(jax.random.fold_in(own, 4), (count // 2,), 0, 1 << 20) % (margin + 1)
    lengths = lengths.at[donor].add(-shifted).at[sink].add(shifted)
    members = jnp.searchsorted(jnp.cumsum(lengths), jnp.arange(rows * top), side="right").astype(jnp.int32)
    grid = members.reshape(top, rows).T
    grid = grid[jax.random.permutation(jax.random.fold_in(own, 1), rows)]
    offset_by = jax.random.randint(jax.random.fold_in(own, 2), (rows, 1), 0, top)
    return jnp.take_along_axis(grid, (jnp.arange(top)[None, :] + offset_by) % top, axis=1)


def load_shares(count, total, bound, skew, full):
    portions = [(1 << 20) // math.isqrt(grade ** skew) + 1 for grade in range(1, count + 1)]
    largest = bound if full else min(bound, max(-(-total // count), total * portions[0] // sum(portions)))
    least = 1 if total - largest >= count - 1 else 0
    holding, spare = [largest] + [least] * (count - 1), total - largest - least * (count - 1)
    while spare > 0:
        free = [i for i in range(1, count) if holding[i] < largest] or [i for i in range(1, count) if holding[i] < bound]
        mass, remaining = sum([portions[i] for i in free]), spare
        for i in free:
            addition = min(bound - holding[i], max(1, remaining * portions[i] // mass), spare)
            holding[i] = holding[i] + addition
            spare = spare - addition
    return np.array(holding)


def gaussian(stream_key, extent, scale, bound, split=(), dtype=jnp.bfloat16):
    level = steps_of(stream_key, extent, split, -0.22, 0.18) if split else 1.0
    values = jax.random.normal(stream_key, extent, jnp.float32) * scale * level
    return jnp.minimum(jnp.maximum(values, -bound), bound).astype(dtype)


def setup_inputs(seed: int = 0) -> dict:
    key_of = jax.random.split(jax.random.key(seed), 8)
    block_values = gaussian(key_of[0], (N_COL, BLOCK_ROWS, BLOCK_LEN), 1.0, 6.0, ((0, 4), (1, 8)))
    block_shifts = jnp.clip(jax.random.uniform(key_of[1], (N_COL, BLOCK_ROWS, BLOCK_LEN), jnp.float32, -1.0, 1.0) * steps_of(key_of[1], (N_COL, BLOCK_ROWS, BLOCK_LEN), ((0, 4), (1, 8)), -0.4, 0.0), -1.0, 1.0).astype(jnp.bfloat16)
    block_sensor = plant(jax.random.randint(key_of[2], (N_COL, BLOCK_ROWS), 0, GROUP_SENSORS), jax.random.fold_in(key_of[2], 1), 0, GROUP_SENSORS - 1).astype(jnp.int32)
    block_window = plant(jax.random.randint(key_of[3], (N_COL, BLOCK_ROWS), 0, WINDOWS), jax.random.fold_in(key_of[3], 1), 0, WINDOWS - 1).astype(jnp.int32)
    block_owner_keys = jax.random.split(jax.random.fold_in(key_of[4], 1), N_COL * BLOCK_ROWS // BLOCKS_DEV)
    block_owner_turns = jax.random.permutation(jax.random.fold_in(key_of[4], 3), N_COL * BLOCK_ROWS // BLOCKS_DEV)
    block_owner = jax.vmap(lambda own, number: deal_out(jax.random.fold_in(key_of[4], 2), own, number, BLOCKS_DEV, N_TM, 1, CAPACITY, 2))(block_owner_keys, block_owner_turns).reshape((N_COL, BLOCK_ROWS, 1))
    block_counts = plant(jax.random.randint(key_of[5], (N_COL, N_TM), 3 * BLOCKS_DEV // 4, BLOCKS_DEV + 1), jax.random.fold_in(key_of[5], 1), 3 * BLOCKS_DEV // 4, BLOCKS_DEV).astype(jnp.int32)
    calibration = gaussian(key_of[6], (SENSORS, OUTPUTS), SENSORS ** -0.5, 0.046875, ((0, 8), (1, 4)))
    return dict(block_values=block_values, block_shifts=block_shifts, block_sensor=block_sensor, block_window=block_window, block_owner=block_owner, block_counts=block_counts, calibration=calibration)


def spread_samples(values, shifts):
    samples = values.astype(jnp.float32)
    offsets = shifts.astype(jnp.float32)
    result = jnp.zeros(samples.shape, jnp.float32)
    lead = [(0, 0)] * (samples.ndim - 1)
    for displace in (-1, 0, 1):
        weight = jnp.maximum(0.0, 1.0 - jnp.abs(offsets - displace)).astype(jnp.bfloat16)
        weight = lax.optimization_barrier(weight).astype(jnp.float32)
        product = weight * samples
        if displace == 1:
            result = result + jnp.pad(product[..., :-1], lead + [(1, 0)])
        elif displace == -1:
            result = result + jnp.pad(product[..., 1:], lead + [(0, 1)])
        else:
            result = result + product
    return result


def reference(block_values, block_shifts, block_sensor, block_window, block_owner, block_counts, calibration):
    length = block_values.shape[2]
    local_index = lax.broadcasted_iota(jnp.int32, (N_COL, BLOCK_ROWS), 1) % BLOCKS_DEV
    counts_rep = jnp.repeat(block_counts, BLOCKS_DEV, axis=1)
    is_live = (local_index < counts_rep).astype(jnp.float32)
    contribution = spread_samples(block_values, block_shifts) * is_live[:, :, None]
    col_base = lax.broadcasted_iota(jnp.int32, (N_COL, BLOCK_ROWS), 0) * GROUP_SENSORS
    row_keys = (block_owner[:, :, 0] * WINDOWS + block_window) * SENSORS + col_base + block_sensor
    summed = jnp.zeros((N_TM * WINDOWS * SENSORS, length), jnp.float32)
    summed = summed.at[row_keys.reshape(-1)].add(contribution.reshape(-1, length))
    aligned = summed.reshape(N_TM * WINDOWS, SENSORS, length).transpose(0, 2, 1)
    aligned = aligned.reshape(GRID_ROWS, SENSORS).astype(jnp.bfloat16)
    return jnp.dot(aligned, calibration, preferred_element_type=jnp.float32).astype(jnp.bfloat16)
```

```python
import functools

import jax
import jax.numpy as jnp
from jax import lax
from jax.experimental import pallas as pl
from jax.experimental.pallas import tpu as pltpu
from jax.sharding import Mesh, PartitionSpec as P

ROWS_DEV = 512
GROUP = 16
KEY_ROWS = 16


def spread_kernel(count_ref, values_ref, shifts_ref, keys_ref, digits_ref, out_ref):
    chunk, length = values_ref.shape
    row = lax.broadcasted_iota(jnp.int32, (length, length), 0)
    lane = lax.broadcasted_iota(jnp.int32, (length, length), 1)
    same_group = (row // GROUP == lane // GROUP) & (lane <= row)
    first = pl.program_id(0) * chunk
    for tile in range(chunk // length):
        at = pl.ds(tile * length, length)
        samples = values_ref[at, :].astype(jnp.float32)
        offsets = shifts_ref[at, :].astype(jnp.float32)

        def weighted(displace):
            weight = jnp.maximum(0.0, 1.0 - jnp.abs(offsets - displace))
            return weight.astype(jnp.bfloat16).astype(jnp.float32) * samples

        before = jnp.where(lane == length - 1, 0.0, pltpu.roll(weighted(-1.0), length - 1, 1))
        after = jnp.where(lane == 0, 0.0, pltpu.roll(weighted(1.0), 1, 1))
        total = before + weighted(0.0) + after
        live = row + (first + tile * length) < count_ref[0, 0]
        total = jnp.where(live, total, 0.0).astype(jnp.bfloat16)
        across = jnp.broadcast_to(keys_ref[0, tile : tile + 1, :], (length, length))
        merge = jnp.where(same_group & (across == across.T), 1.0, 0.0).astype(jnp.bfloat16)
        merged = jnp.dot(merge, total, preferred_element_type=jnp.float32)
        out_ref[0, at, :] = merged.astype(jnp.bfloat16)
    out_ref[0, pl.ds(chunk, KEY_ROWS), :] = digits_ref[0]


def spread_blocks(count, values, shifts, keys, parts):
    blocks, length = values.shape
    chunk = blocks // parts
    lines = chunk // length
    keys = keys.reshape(parts, lines, length)
    digits = jnp.stack([keys & 255, (keys >> 8) & 255, keys >> 16], axis=1)
    digits = digits.reshape(parts, 3 * lines, length).astype(jnp.bfloat16)
    digits = jnp.pad(digits, ((0, 0), (0, KEY_ROWS - 3 * lines), (0, 0)))
    return pl.pallas_call(
        spread_kernel,
        grid=(parts,),
        out_shape=jax.ShapeDtypeStruct((parts, chunk + KEY_ROWS, length), jnp.bfloat16),
        in_specs=[
            pl.BlockSpec(memory_space=pltpu.SMEM),
            pl.BlockSpec((chunk, length), lambda i: (i, 0)),
            pl.BlockSpec((chunk, length), lambda i: (i, 0)),
            pl.BlockSpec((1, lines, length), lambda i: (i, 0, 0)),
            pl.BlockSpec((1, KEY_ROWS, length), lambda i: (i, 0, 0)),
        ],
        out_specs=pl.BlockSpec((1, chunk + KEY_ROWS, length), lambda i: (i, 0, 0)),
        name="spread",
    )(count, values, shifts, keys.astype(jnp.float32), digits)


def scatter_kernel(pieces, index_ref, *refs):
    piece_refs, (out_ref, total) = refs[:pieces], refs[pieces:]
    spare = total.shape[0] - 8
    sensors = out_ref.shape[1]
    step = pl.program_id(0)

    @pl.when(step == 0)
    def _():
        def clear(i, carry):
            total[pl.ds(i * 256, 256), :] = jnp.zeros((256, total.shape[1]), jnp.float32)
            return carry

        lax.fori_loop(0, spare // 256, clear, 0)
        total[pl.ds(spare, 8), :] = jnp.zeros((8, total.shape[1]), jnp.float32)
        done = 0
        for piece in piece_refs:
            parts, rows = piece.shape[0], piece.shape[1] - KEY_ROWS
            for part in range(parts):

                def add(i, carry, piece=piece, part=part, base=done):
                    start = i * GROUP
                    places = [index_ref[base + start + j] for j in range(GROUP)]
                    block = piece[part, pl.ds(pl.multiple_of(start, GROUP), GROUP), :]
                    block = block.astype(jnp.float32)
                    sums = [
                        total[pl.ds(places[j], 1), :] + block[j : j + 1, :] for j in range(GROUP)
                    ]
                    for j in range(GROUP):
                        total[pl.ds(places[j], 1), :] = sums[j]
                    return carry

                lax.fori_loop(0, rows // GROUP, add, 0)
                done += rows

    at = pl.ds(pl.multiple_of(step * sensors, sensors), sensors)
    out_ref[0, :, :] = total[at, :].astype(jnp.bfloat16)


def scatter_blocks(index, pieces, owners, panels, sensors):
    length = pieces[0].shape[2]
    rows = owners * panels * sensors
    whole = pl.BlockSpec(pieces[0].shape, lambda i: (0, 0, 0))
    return pl.pallas_call(
        functools.partial(scatter_kernel, len(pieces)),
        grid=(owners * panels,),
        out_shape=jax.ShapeDtypeStruct((owners, sensors, panels * length), jnp.bfloat16),
        in_specs=[pl.BlockSpec(memory_space=pltpu.SMEM)] + [whole] * len(pieces),
        out_specs=pl.BlockSpec((1, sensors, length), lambda i: (i // panels, 0, i % panels)),
        scratch_shapes=[pltpu.VMEM((rows + 8, length), jnp.float32)],
        compiler_params=pltpu.CompilerParams(vmem_limit_bytes=60 << 20),
        name="scatter",
    )(index, *pieces)


def per_device(values, shifts, sensor, window, owner, counts, calibration):
    ring, halves, group_count = lax.axis_size("g"), lax.axis_size("h"), lax.axis_size("col")
    values, shifts = values[0], shifts[0]
    blocks, length = values.shape
    sensors, outputs = calibration.shape
    group_sensors = halves * sensors
    windows = ROWS_DEV // length
    chunk = blocks // group_count
    lines = chunk // length
    my_ring, my_half = lax.axis_index("g"), lax.axis_index("h")

    keys = (owner[0, :, 0] * windows + window[0]) * group_sensors + sensor[0]
    routed = spread_blocks(counts, values, shifts, keys, group_count)
    routed = lax.all_to_all(routed, "col", split_axis=0, concat_axis=0, tiled=True)
    routed = lax.all_to_all(routed, "g", split_axis=0, concat_axis=0, tiled=True)

    def flipped(name, bit):
        return [(i, i ^ bit) for i in range(lax.axis_size(name))]

    def doubled(held, name, bit):
        return held + [lax.ppermute(x, name, flipped(name, bit)) for x in held]

    col_bits = [1 << b for b in reversed(range(1, (group_count - 1).bit_length()))]
    first, second = [routed[: ring // 2]], [routed[ring // 2 :]]
    first = doubled(first, "h", 1)
    for bit in col_bits:
        first, second = doubled(first, "col", bit), doubled(second, "col", bit)
    second = doubled(second, "h", 1)
    pieces = doubled(first, "col", 1) + doubled(second, "col", 1)

    digits = jnp.stack([x[:, chunk : chunk + 3 * lines] for x in pieces])
    digits = digits.reshape(-1, 3, lines, length).astype(jnp.float32).astype(jnp.int32)
    key = (digits[:, 0] + digits[:, 1] * 256 + digits[:, 2] * 65536).reshape(-1)
    to_sensor, to_panel = key % group_sensors, key // group_sensors
    to_owner, to_window = to_panel // windows, to_panel % windows
    to_ring = (to_owner // halves - my_ring + ring) % ring
    panel = (to_ring * halves + to_owner % halves) * windows + to_window
    panels = halves * windows
    index = jnp.where(
        to_sensor // sensors == my_half,
        panel * sensors + to_sensor % sensors,
        ring * panels * sensors,
    )
    aligned = scatter_blocks(index, pieces, ring, panels, sensors)

    def partial(distance):
        return lax.optimization_barrier(
            lax.dot_general(
                aligned[distance % ring],
                calibration,
                (((0,), (0,)), ((), ())),
                preferred_element_type=jnp.float32,
            ).astype(jnp.bfloat16)
        )

    def add(a, b):
        return (a.astype(jnp.float32) + b.astype(jnp.float32)).astype(jnp.bfloat16)

    ahead = [(i, (i + 1) % ring) for i in range(ring)]
    back = [(i, (i - 1) % ring) for i in range(ring)]
    split = outputs // 2
    far = partial(ring // 2)
    up = [lax.ppermute(far[:, :split], "g", ahead)]
    down = [lax.ppermute(far[:, split:], "g", back)]
    for distance in range(ring // 2 - 1, 0, -1):
        rise, fall = partial(distance), partial(-distance)
        rise_parts, fall_parts = [rise[:, :split], rise[:, split:]], [fall[:, split:], fall[:, :split]]
        up = [lax.ppermute(add(rise_parts[i], up[i]) if i < len(up) else rise_parts[i], "g", ahead) for i in range(2)]
        down = [lax.ppermute(add(fall_parts[i], down[i]) if i < len(down) else fall_parts[i], "g", back) for i in range(2)]
    here = partial(0)
    total = (
        here.astype(jnp.float32)
        + jnp.concatenate(up, axis=1).astype(jnp.float32)
        + jnp.concatenate(down[::-1], axis=1).astype(jnp.float32)
    )
    total = total.astype(jnp.bfloat16).reshape(halves, ROWS_DEV, outputs)
    mine = lax.dynamic_index_in_dim(total, my_half, 0, keepdims=False)
    other = lax.dynamic_index_in_dim(total, 1 - my_half, 0, keepdims=False)
    return add(mine, lax.ppermute(other, "h", flipped("h", 1)))


def solution(mesh):
    rows, cols = mesh.devices.shape
    if rows != 2 * cols:
        raise ValueError("mesh shape")
    split_mesh = Mesh(mesh.devices.reshape(cols, 2, cols), ("g", "h", "col"))
    time = ("g", "h")
    placed = (
        P("col", time, None),
        P("col", time, None),
        P("col", time),
        P("col", time),
        P("col", time, None),
        P("col", time),
        P(time, "col"),
    )
    return jax.shard_map(
        per_device, mesh=split_mesh, in_specs=placed, out_specs=P(time, "col"), check_vma=False
    )
```

```python
import functools

import jax
import jax.numpy as jnp
from jax import lax
from jax.experimental import pallas as pl
from jax.experimental.pallas import tpu as pltpu
from jax.sharding import Mesh, PartitionSpec as P

ROWS_DEV = 512
GROUP = 16
KEY_ROWS = 16
CHUNKS = 2


def spread_kernel(count_ref, values_ref, shifts_ref, keys_ref, digits_ref, out_ref):
    chunk, length = values_ref.shape
    row = lax.broadcasted_iota(jnp.int32, (length, length), 0)
    lane = lax.broadcasted_iota(jnp.int32, (length, length), 1)
    same_group = (row // GROUP == lane // GROUP) & (lane <= row)
    first = pl.program_id(0) * chunk
    for tile in range(chunk // length):
        at = pl.ds(tile * length, length)
        samples = values_ref[at, :].astype(jnp.float32)
        offsets = shifts_ref[at, :].astype(jnp.float32)

        def weighted(displace):
            weight = jnp.maximum(0.0, 1.0 - jnp.abs(offsets - displace))
            return weight.astype(jnp.bfloat16).astype(jnp.float32) * samples

        before = jnp.where(lane == length - 1, 0.0, pltpu.roll(weighted(-1.0), length - 1, 1))
        after = jnp.where(lane == 0, 0.0, pltpu.roll(weighted(1.0), 1, 1))
        total = before + weighted(0.0) + after
        live = row + (first + tile * length) < count_ref[0, 0]
        total = jnp.where(live, total, 0.0).astype(jnp.bfloat16)
        across = jnp.broadcast_to(keys_ref[0, tile : tile + 1, :], (length, length))
        merge = jnp.where(same_group & (across == across.T), 1.0, 0.0).astype(jnp.bfloat16)
        merged = jnp.dot(merge, total, preferred_element_type=jnp.float32)
        out_ref[0, at, :] = merged.astype(jnp.bfloat16)
    out_ref[0, pl.ds(chunk, KEY_ROWS), :] = digits_ref[0]


def spread_blocks(count, values, shifts, keys, parts):
    blocks, length = values.shape
    chunk = blocks // parts
    lines = chunk // length
    keys = keys.reshape(parts, lines, length)
    digits = jnp.stack([keys & 255, (keys >> 8) & 255, keys >> 16], axis=1)
    digits = digits.reshape(parts, 3 * lines, length).astype(jnp.bfloat16)
    digits = jnp.pad(digits, ((0, 0), (0, KEY_ROWS - 3 * lines), (0, 0)))
    return pl.pallas_call(
        spread_kernel,
        grid=(parts,),
        out_shape=jax.ShapeDtypeStruct((parts, chunk + KEY_ROWS, length), jnp.bfloat16),
        in_specs=[
            pl.BlockSpec(memory_space=pltpu.SMEM),
            pl.BlockSpec((chunk, length), lambda i: (i, 0)),
            pl.BlockSpec((chunk, length), lambda i: (i, 0)),
            pl.BlockSpec((1, lines, length), lambda i: (i, 0, 0)),
            pl.BlockSpec((1, KEY_ROWS, length), lambda i: (i, 0, 0)),
        ],
        out_specs=pl.BlockSpec((1, chunk + KEY_ROWS, length), lambda i: (i, 0, 0)),
        name="spread",
    )(count, values, shifts, keys.astype(jnp.float32), digits)


def scatter_kernel(pieces, index_ref, *refs):
    piece_refs, (out_ref, total) = refs[:pieces], refs[pieces:]
    spare = total.shape[0] - 8
    sensors = out_ref.shape[1]
    step = pl.program_id(0)

    @pl.when(step == 0)
    def _():
        def clear(i, carry):
            total[pl.ds(i * 256, 256), :] = jnp.zeros((256, total.shape[1]), jnp.float32)
            return carry

        lax.fori_loop(0, spare // 256, clear, 0)
        total[pl.ds(spare, 8), :] = jnp.zeros((8, total.shape[1]), jnp.float32)
        done = 0
        for piece in piece_refs:
            parts, rows = piece.shape[0], piece.shape[1] - KEY_ROWS
            for part in range(parts):

                def add(i, carry, piece=piece, part=part, base=done):
                    start = i * GROUP
                    places = [index_ref[base + start + j] for j in range(GROUP)]
                    block = piece[part, pl.ds(pl.multiple_of(start, GROUP), GROUP), :]
                    block = block.astype(jnp.float32)
                    sums = [
                        total[pl.ds(places[j], 1), :] + block[j : j + 1, :] for j in range(GROUP)
                    ]
                    for j in range(GROUP):
                        total[pl.ds(places[j], 1), :] = sums[j]
                    return carry

                lax.fori_loop(0, rows // GROUP, add, 0)
                done += rows

    at = pl.ds(pl.multiple_of(step * sensors, sensors), sensors)
    out_ref[0, :, :] = total[at, :].astype(jnp.bfloat16)


def scatter_blocks(index, pieces, owners, panels, sensors):
    length = pieces[0].shape[2]
    rows = owners * panels * sensors
    whole = pl.BlockSpec(pieces[0].shape, lambda i: (0, 0, 0))
    return pl.pallas_call(
        functools.partial(scatter_kernel, len(pieces)),
        grid=(owners * panels,),
        out_shape=jax.ShapeDtypeStruct((owners, sensors, panels * length), jnp.bfloat16),
        in_specs=[pl.BlockSpec(memory_space=pltpu.SMEM)] + [whole] * len(pieces),
        out_specs=pl.BlockSpec((1, sensors, length), lambda i: (i // panels, 0, i % panels)),
        scratch_shapes=[pltpu.VMEM((rows + 8, length), jnp.float32)],
        compiler_params=pltpu.CompilerParams(vmem_limit_bytes=60 << 20),
        name="scatter",
    )(index, *pieces)


def per_device(values, shifts, sensor, window, owner, counts, calibration):
    ring, halves, group_count = lax.axis_size("g"), lax.axis_size("h"), lax.axis_size("col")
    values, shifts = values[0], shifts[0]
    blocks, length = values.shape
    sensors, outputs = calibration.shape
    group_sensors = halves * sensors
    windows = ROWS_DEV // length
    chunk = blocks // group_count
    lines = chunk // length
    my_ring, my_half = lax.axis_index("g"), lax.axis_index("h")

    def flipped(name, bit):
        return [(i, i ^ bit) for i in range(lax.axis_size(name))]

    split = outputs // CHUNKS
    own_parts = [calibration[:, i * split : (i + 1) * split] for i in range(CHUNKS)]
    other_parts = [lax.ppermute(own_parts[0], "h", flipped("h", 1))]

    keys = (owner[0, :, 0] * windows + window[0]) * group_sensors + sensor[0]
    routed = spread_blocks(counts, values, shifts, keys, group_count)
    routed = lax.all_to_all(routed, "col", split_axis=0, concat_axis=0, tiled=True)
    routed = lax.all_to_all(routed, "g", split_axis=0, concat_axis=0, tiled=True)

    def doubled(held, name, bit):
        return held + [lax.ppermute(x, name, flipped(name, bit)) for x in held]

    col_bits = [1 << b for b in reversed(range(1, (group_count - 1).bit_length()))]
    first, second = [routed[: ring // 2]], [routed[ring // 2 :]]
    first = doubled(first, "h", 1)
    for bit in col_bits:
        first, second = doubled(first, "col", bit), doubled(second, "col", bit)
    second = doubled(second, "h", 1)
    second, own_parts[1:] = lax.optimization_barrier((second, own_parts[1:]))
    other_parts += [lax.ppermute(x, "h", flipped("h", 1)) for x in own_parts[1:]]
    pieces = doubled(first, "col", 1) + doubled(second, "col", 1)

    digits = jnp.stack([x[:, chunk : chunk + 3 * lines] for x in pieces])
    digits = digits.reshape(-1, 3, lines, length).astype(jnp.float32).astype(jnp.int32)
    key = (digits[:, 0] + digits[:, 1] * 256 + digits[:, 2] * 65536).reshape(-1)
    to_sensor, to_panel = key % group_sensors, key // group_sensors
    to_owner, to_window = to_panel // windows, to_panel % windows
    to_ring = (to_owner // halves - my_ring + ring) % ring
    place = (to_sensor // sensors + my_half) % halves * sensors + to_sensor % sensors
    index = jnp.where(
        to_owner % halves == my_half,
        (to_ring * windows + to_window) * group_sensors + place,
        ring * windows * group_sensors,
    )
    aligned = scatter_blocks(index, pieces, ring, windows, group_sensors)

    def full(part):
        return jnp.concatenate([own_parts[part], other_parts[part]], axis=0)

    whole = [full(part) for part in range(CHUNKS)]

    def partial(distance, part):
        return lax.optimization_barrier(
            lax.dot_general(
                aligned[distance % ring],
                whole[part],
                (((0,), (0,)), ((), ())),
                preferred_element_type=jnp.float32,
            ).astype(jnp.bfloat16)
        )

    def add(a, b):
        return (a.astype(jnp.float32) + b.astype(jnp.float32)).astype(jnp.bfloat16)

    partials = {}
    for distance in list(range(ring - 1, 0, -1)) + [0]:
        for part in range(CHUNKS):
            for sign in (1, -1):
                at = (sign * distance % ring, part)
                if at not in partials:
                    partials[at] = partial(*at)
    right, left = [None] * CHUNKS, [None] * CHUNKS
    for distance in range(ring - 1, 0, -1):
        ahead = [(i, i + 1) for i in range(ring - distance)]
        back = [(i, i - 1) for i in range(distance, ring)]
        for part in range(CHUNKS):
            rise, fall = partials[distance, part], partials[-distance % ring, part]
            if right[part] is not None:
                rise, fall = add(rise, right[part]), add(fall, left[part])
            right[part] = lax.ppermute(rise, "g", ahead)
            left[part] = lax.ppermute(fall, "g", back)
    total = [
        (
            partials[0, part].astype(jnp.float32)
            + right[part].astype(jnp.float32)
            + left[part].astype(jnp.float32)
        ).astype(jnp.bfloat16)
        for part in range(CHUNKS)
    ]
    return jnp.concatenate(total, axis=1)


def solution(mesh):
    rows, cols = mesh.devices.shape
    if rows != 2 * cols:
        raise ValueError("mesh shape")
    split_mesh = Mesh(mesh.devices.reshape(cols, 2, cols), ("g", "h", "col"))
    time = ("g", "h")
    placed = (
        P("col", time, None),
        P("col", time, None),
        P("col", time),
        P("col", time),
        P("col", time, None),
        P("col", time),
        P(time, "col"),
    )
    return jax.shard_map(
        per_device, mesh=split_mesh, in_specs=placed, out_specs=P(time, "col"), check_vma=False
    )
```

```python
import functools

import jax
import jax.numpy as jnp
from jax import lax
from jax.experimental import pallas as pl
from jax.experimental.pallas import tpu as pltpu
from jax.sharding import Mesh, PartitionSpec as P


ROWS_DEV = 512
GROUP = 16
KEY_ROWS = 16
CHUNKS = 4


def spread_kernel(values_ref, shifts_ref, rank_ref, digits_ref, out_ref, spread, lines_ref):
    chunk, length = values_ref.shape
    lines = chunk // length
    classes = lines_ref.shape[0]
    row = lax.broadcasted_iota(jnp.int32, (length, length), 0)
    lane = lax.broadcasted_iota(jnp.int32, (length, length), 1)
    same_group = (row // GROUP == lane // GROUP) & (lane <= row)
    for tile in range(lines):
        at = pl.ds(tile * length, length)
        samples = values_ref[at, :].astype(jnp.float32)
        offsets = shifts_ref[at, :].astype(jnp.float32)

        def weighted(displace):
            weight = jnp.maximum(0.0, 1.0 - jnp.abs(offsets - displace))
            return weight.astype(jnp.bfloat16).astype(jnp.float32) * samples

        before = jnp.where(lane == length - 1, 0.0, pltpu.roll(weighted(-1.0), length - 1, 1))
        after = jnp.where(lane == 0, 0.0, pltpu.roll(weighted(1.0), 1, 1))
        spread[at, :] = (before + weighted(0.0) + after).astype(jnp.bfloat16)

    rank = rank_ref[0]
    number = lax.broadcasted_iota(jnp.int32, (classes, chunk), 0)
    member = jnp.where(number == rank, 1.0, 0.0)
    start = jnp.sum(jnp.where(rank < number, 1.0, 0.0), axis=1, keepdims=True)
    slot = lax.broadcasted_iota(jnp.int32, (chunk, chunk), 0)
    other = lax.broadcasted_iota(jnp.int32, (chunk, chunk), 1)
    earlier = jnp.where(slot < other, 1.0, 0.0).astype(jnp.bfloat16)
    before = jnp.dot(member.astype(jnp.bfloat16), earlier, preferred_element_type=jnp.float32)
    place = jnp.sum(member * (before + start), axis=0, keepdims=True).astype(jnp.int32)
    order = jnp.where(slot == place, 1.0, 0.0).astype(jnp.bfloat16)
    blocks = jnp.dot(order, spread[...], preferred_element_type=jnp.float32).astype(jnp.bfloat16)
    digits = lax.dot_general(
        digits_ref[0], order, (((1,), (1,)), ((), ())), preferred_element_type=jnp.float32
    )
    key = digits[0:1] + digits[1:2] * 256.0 + digits[2:3] * 65536.0
    for tile in range(lines):
        at = slice(tile * length, (tile + 1) * length)
        across = jnp.broadcast_to(key[:, at], (length, length))
        merge = jnp.where(same_group & (across == across.T), 1.0, 0.0).astype(jnp.bfloat16)
        merged = jnp.dot(merge, blocks[at], preferred_element_type=jnp.float32)
        out_ref[0, pl.ds(tile * length, length), :] = merged.astype(jnp.bfloat16)
        for digit in range(3):
            at_line = pl.ds(digit * lines + tile, 1)
            lines_ref[at_line, :] = digits[digit : digit + 1, at]
    narrow = lax.broadcasted_iota(jnp.int32, (classes, length), 0)
    wide = lax.broadcasted_iota(jnp.int32, (classes, length), 1)
    starts = jnp.sum(jnp.where(narrow == wide, start, 0.0), axis=0, keepdims=True).astype(jnp.int32)
    lines_ref[pl.ds(3 * lines, 1), :] = (starts & 255).astype(jnp.float32)
    lines_ref[pl.ds(3 * lines + 1, 1), :] = (starts >> 8).astype(jnp.float32)
    out_ref[0, pl.ds(chunk, KEY_ROWS), :] = lines_ref[0:KEY_ROWS, :].astype(jnp.bfloat16)


def spread_blocks(values, shifts, ranks, keys, parts, owners):
    blocks, length = values.shape
    chunk = blocks // parts
    classes = max(-(-(owners + 1) // 8) * 8, KEY_ROWS)
    keys = keys.reshape(parts, 1, chunk)
    digits = jnp.concatenate([keys & 255, (keys >> 8) & 255, keys >> 16], axis=1)
    digits = jnp.pad(digits, ((0, 0), (0, 13), (0, 0))).astype(jnp.bfloat16)
    return pl.pallas_call(
        spread_kernel,
        grid=(parts,),
        out_shape=jax.ShapeDtypeStruct((parts, chunk + KEY_ROWS, length), jnp.bfloat16),
        in_specs=[
            pl.BlockSpec((chunk, length), lambda i: (i, 0)),
            pl.BlockSpec((chunk, length), lambda i: (i, 0)),
            pl.BlockSpec((1, 1, chunk), lambda i: (i, 0, 0)),
            pl.BlockSpec((1, 16, chunk), lambda i: (i, 0, 0)),
        ],
        out_specs=pl.BlockSpec((1, chunk + KEY_ROWS, length), lambda i: (i, 0, 0)),
        scratch_shapes=[
            pltpu.VMEM((chunk, length), jnp.bfloat16),
            pltpu.VMEM((classes, length), jnp.float32),
        ],
        cost_estimate=pl.CostEstimate(
            flops=8 * blocks * chunk * length, bytes_accessed=6 * blocks * length, transcendentals=0
        ),
        name="spread",
    )(values, shifts, ranks.reshape(parts, 1, chunk), digits)


def scatter_kernel(pieces, windows, distance, where_ref, *refs):
    piece_refs = refs[:pieces]
    out_ref, total, index_v, table_v, index_s, table_s, sems = refs[pieces:]
    sensors = out_ref.shape[0]
    length = total.shape[1]
    spare = windows * sensors
    half = sensors // 2
    parts, rows = piece_refs[0].shape[0], piece_refs[0].shape[1] - KEY_ROWS
    lines = rows // length
    owner = where_ref[distance]
    my_half = where_ref[where_ref.shape[0] - 1]
    step = pl.program_id(0)

    @pl.when(step == 0)
    def _():
        for number in range(pieces * parts):
            piece, part = piece_refs[number // parts], number % parts
            digits = piece[part, pl.ds(rows, KEY_ROWS), :].astype(jnp.float32).astype(jnp.int32)
            key = digits[0:lines] + (digits[lines : 2 * lines] << 8)
            key = key + (digits[2 * lines : 3 * lines] << 16)
            sensor, panel = key & (sensors - 1), key >> (sensors.bit_length() - 1)
            window = panel & (windows - 1)
            row = window * sensors + (sensor ^ (my_half * half))
            match = (panel >> (windows.bit_length() - 1)) == owner
            index_v[pl.ds(number * lines, lines), :] = jnp.where(match, row, spare)
            low, high = digits[3 * lines : 3 * lines + 1], digits[3 * lines + 1 : 3 * lines + 2]
            table_v[pl.ds(number, 1), :] = low + (high << 8)
        copies = [
            pltpu.make_async_copy(index_v, index_s, sems.at[0]),
            pltpu.make_async_copy(table_v, table_s, sems.at[1]),
        ]
        for copy in copies:
            copy.start()

        def clear(i, carry):
            total[pl.ds(i * 256, 256), :] = jnp.zeros((256, length), jnp.float32)
            return carry

        lax.fori_loop(0, spare // 256, clear, 0)
        total[pl.ds(spare, 8), :] = jnp.zeros((8, length), jnp.float32)
        for copy in copies:
            copy.wait()
        for place, piece in enumerate(piece_refs):

            def run(part, carry, piece=piece, place=place):
                number = place * parts + part

                def add(i, carry):
                    start = i * GROUP
                    at_line, at_lane = number * lines + start // length, start % length
                    places = [index_s[at_line, at_lane + j] for j in range(GROUP)]
                    block = piece[part, pl.ds(pl.multiple_of(start, GROUP), GROUP), :]
                    block = block.astype(jnp.float32)
                    sums = [
                        total[pl.ds(places[j], 1), :] + block[j : j + 1, :] for j in range(GROUP)
                    ]
                    for j in range(GROUP):
                        total[pl.ds(places[j], 1), :] = sums[j]
                    return carry

                low, high = table_s[number, owner], table_s[number, owner + 1]
                lax.fori_loop(low // GROUP, (high + GROUP - 1) // GROUP, add, 0)
                return carry

            lax.fori_loop(0, parts, run, 0)

    at = pl.ds(pl.multiple_of(step * sensors, sensors), sensors)
    out_ref[...] = total[at, :].astype(jnp.bfloat16)


def scatter_blocks(where, pieces, windows, sensors, distance):
    parts, rows, length = pieces[0].shape
    lines = (rows - KEY_ROWS) // length
    numbers = len(pieces) * parts
    whole = pl.BlockSpec(pieces[0].shape, lambda i: (0, 0, 0))
    return pl.pallas_call(
        functools.partial(scatter_kernel, len(pieces), windows, distance),
        grid=(windows,),
        out_shape=jax.ShapeDtypeStruct((sensors, windows * length), jnp.bfloat16),
        in_specs=[pl.BlockSpec(memory_space=pltpu.SMEM)] + [whole] * len(pieces),
        out_specs=pl.BlockSpec((sensors, length), lambda i: (0, i)),
        scratch_shapes=[
            pltpu.VMEM((windows * sensors + 8, length), jnp.float32),
            pltpu.VMEM((numbers * lines, length), jnp.int32),
            pltpu.VMEM((numbers, length), jnp.int32),
            pltpu.SMEM((numbers * lines, length), jnp.int32),
            pltpu.SMEM((numbers, length), jnp.int32),
            pltpu.SemaphoreType.DMA((2,)),
        ],
        compiler_params=pltpu.CompilerParams(vmem_limit_bytes=40 << 20),
        cost_estimate=pl.CostEstimate(
            flops=4 * sensors * windows * length * 1000,
            bytes_accessed=12 << 20,
            transcendentals=0,
        ),
        name="scatter",
    )(where, *pieces)


def per_device(values, shifts, sensor, window, owner, counts, calibration):
    ring, halves, group_count = lax.axis_size("g"), lax.axis_size("h"), lax.axis_size("col")
    values, shifts = values[0], shifts[0]
    blocks, length = values.shape
    sensors, outputs = calibration.shape
    group_sensors = halves * sensors
    windows = ROWS_DEV // length
    my_ring, my_half = lax.axis_index("g"), lax.axis_index("h")
    owners = ring * halves

    def flipped(name, bit):
        return [(i, i ^ bit) for i in range(lax.axis_size(name))]

    split = outputs // CHUNKS
    own_parts = [calibration[:, i * split : (i + 1) * split] for i in range(CHUNKS)]
    other_parts = [lax.ppermute(own_parts[0], "h", flipped("h", 1))]

    ranks = jnp.where(lax.iota(jnp.int32, blocks) < counts[0, 0], owner[0, :, 0], owners)
    keys = (ranks * windows + window[0]) * group_sensors + sensor[0]
    routed = spread_blocks(values, shifts, ranks, keys, group_count, owners)

    def moved(part):
        pairs = [
            (g * group_count + c, c * group_count + (g ^ part))
            for g in range(ring)
            for c in range(group_count)
        ]
        return lax.ppermute(routed[part], ("g", "col"), pairs)

    held = [moved(part) for part in range(group_count)]
    count = group_count // 2
    first, second = [jnp.stack(held[:count])], [jnp.stack(held[count:])]

    def doubled(held, name, bit):
        return held + [lax.ppermute(x, name, flipped(name, bit)) for x in held]

    col_bits = [1 << b for b in reversed(range(1, (group_count - 1).bit_length()))]
    first = doubled(first, "h", 1)
    for bit in col_bits:
        first, second = doubled(first, "col", bit), doubled(second, "col", bit)
    second = doubled(second, "h", 1)
    second, own_parts[1:] = lax.optimization_barrier((second, own_parts[1:]))
    other_parts += [lax.ppermute(x, "h", flipped("h", 1)) for x in own_parts[1:]]
    pieces = doubled(first, "col", 1) + doubled(second, "col", 1)

    fold = ring == 4
    sign = jnp.where(my_ring < ring // 2, 1, -1) if fold else 1
    distances = lax.iota(jnp.int32, ring)
    where = (my_ring + sign * distances + ring) % ring * halves + my_half
    where = jnp.concatenate([where, my_half[None]])

    def full(part):
        return jnp.concatenate([own_parts[part], other_parts[part]], axis=0)

    whole = [full(part) for part in range(CHUNKS)]

    def scattered(at):
        return scatter_blocks(where, pieces, windows, group_sensors, at)

    def partial(at, part):
        out = lax.dot_general(
            aligned[at],
            whole[part],
            (((0,), (0,)), ((), ())),
            preferred_element_type=jnp.float32,
        ).astype(jnp.bfloat16)
        return lax.optimization_barrier(out)

    def add(a, b):
        return (a.astype(jnp.float32) + b.astype(jnp.float32)).astype(jnp.bfloat16)

    def sent(x, pairs):
        return lax.ppermute(x, "g", pairs)

    aligned, partials = {}, {}
    for at in range(ring - 1, -1, -1):
        aligned[at] = scattered(at)
        partials[at, 0] = partial(at, 0)
        partials[at, 0], where = lax.optimization_barrier((partials[at, 0], where))
    last = partials[0, 0]
    for part in range(1, CHUNKS):
        for at in range(ring - 1, -1, -1):
            last, whole[part] = lax.optimization_barrier((last, whole[part]))
            if at == ring - 1:
                partials[0, part - 1] = last
            else:
                partials[at + 1, part] = last
            last = partials[at, part] = partial(at, part)

    total = []
    for part in range(CHUNKS):
        here = partials[0, part].astype(jnp.float32)
        if fold:
            inward, across, outward = [(0, 1), (3, 2)], [(1, 2), (2, 1)], [(1, 0), (2, 3)]
            far = sent(partials[3, part], inward)
            mid = sent(partials[2, part], inward)
            near = sent(partials[1, part], inward)
            cross = sent(add(partials[2, part], far), across)
            come = sent(add(partials[1, part], mid), across)
            end = sent(add(partials[3, part], cross), outward)
            for x in (near, come, end):
                here = here + x.astype(jnp.float32)
        else:
            right = left = None
            for distance in range(ring - 1, 0, -1):
                ahead = [(i, i + 1) for i in range(ring - distance)]
                back = [(i, i - 1) for i in range(distance, ring)]
                rise, fall = partials[distance, part], partials[-distance % ring, part]
                if right is not None:
                    rise, fall = add(rise, right), add(fall, left)
                right, left = sent(rise, ahead), sent(fall, back)
            here = here + right.astype(jnp.float32) + left.astype(jnp.float32)
        total.append(here.astype(jnp.bfloat16))
    return jnp.concatenate(total, axis=1)


def solution(mesh):
    rows, cols = mesh.devices.shape
    if rows != 2 * cols:
        raise ValueError("mesh shape")
    split_mesh = Mesh(mesh.devices.reshape(cols, 2, cols), ("g", "h", "col"))
    time = ("g", "h")
    placed = (
        P("col", time, None),
        P("col", time, None),
        P("col", time),
        P("col", time),
        P("col", time, None),
        P("col", time),
        P(time, "col"),
    )
    return jax.shard_map(
        per_device, mesh=split_mesh, in_specs=placed, out_specs=P(time, "col"), check_vma=False
    )
```
